512 devices in a mesh: freq: 4 (over x), row: 16 (over y, z_hi, core), col: 8 (over z_lo).
Axes of the slice: x: 4, y: 4, z: 16 (z_hi: 2, z_lo: 8; z = z_hi * 8 + z_lo), core: 2. Of those that a mesh axis runs over, the one named last changes fastest.
Arguments:
- pair_block: bfloat16 [768, 8192], P('freq', 'row'), may hold values from -6 to 6
- screened: bfloat16 [16, 8192, 8192], P('freq', 'row', 'col'), may hold values from -0.0625 to 0.0625
- pair_gaps: float32 [768], replicated, may hold values from 0.5 to 4
- omega_values: float32 [16], replicated, may hold values from 0.25 to 8
- quad_weight: float32 [16], replicated, may hold values from 0.2 to 1
- freq_slot: int32 [16], replicated, may hold values from 0 to 15, each once
- block_list: int32 [64], replicated, may hold values from 0 to 63, each once
Outputs:
- gamma: float32 [768, 8192], P(('freq', 'row'), 'col')
The draws below stay inside these ranges and needn't reach their ends.
Inputs may be any that keep to these rules, and one draw needn't show every extreme that they name: `freq_slot`: a permutation of the frequencies. `block_list`: a permutation of the blocks.
All inputs are finite; a program needn't handle non-finite values.
Results may differ from the reference program's by a relative error of at most 0.0003.
Values may be sent and summed in bfloat16 or wider, within the bound.
A program may use at most 64 MiB of HBM per device.

```python
import math
import jax
import jax.numpy as jnp
from jax import lax

NAUX = 8192
PAIRS = 768
NFREQ = 16
NBLK = 64


def with_spikes(drawn, rng, source, target, blocks, factor):
    owner, partner = [(jnp.arange(drawn.shape[position]) // (drawn.shape[position] // blocks)).reshape([-1 if axis == position else 1 for axis in range(drawn.ndim)]) for position in (source, target)]
    chosen = jax.random.permutation(rng, blocks)[partner]
    strong = (owner == chosen) | (owner == (partner + blocks // 2) % blocks)
    return jnp.where(strong, factor * drawn, drawn)


def level_of(rng, dims, shards, low, top_value):
    def one(position, blocks):
        draws = jax.random.uniform(jax.random.fold_in(jax.random.fold_in(rng, 6), position), (blocks,), jnp.float32, low / len(shards), top_value / len(shards))
        return jnp.repeat(jnp.exp(draws), dims[position] // blocks).reshape((-1,) + (1,) * (len(dims) - position - 1))

    gain = one(*shards[0])
    for cut in shards[1:]:
        gain = gain * one(*cut)
    return gain


def centred(rng, dims, spread, limit, shards=(), held_as=jnp.bfloat16):
    array = spread * jax.random.normal(rng, dims, jnp.float32)
    if shards:
        array = array * level_of(rng, dims, shards, -0.22, 0.18)
    return jnp.clip(array, -limit, limit).astype(held_as)


def bell_draw_with(rng, shape, deviation, bound, shards, heavy, kind=jnp.bfloat16):
    values = deviation * jax.random.normal(rng, shape, jnp.float32)
    if shards:
        values = values * level_of(rng, shape, shards, -0.22, 0.18)
    return jnp.clip(with_spikes(values, jax.random.fold_in(rng, 3), *heavy), -bound, bound).astype(kind)


def setup_inputs(seed: int = 0) -> dict:
    seeds = jax.random.split(jax.random.key(seed), 8)
    pair_block = bell_draw_with(seeds[0], (PAIRS, NAUX), 1.0, 6.0, ((0, 4), (1, 16)), (1, 0, 16, 2.0))
    screened = centred(seeds[1], (NFREQ, NAUX, NAUX), NAUX ** -0.5, 0.0625, ((0, 4), (1, 16), (2, 8)))
    pair_gaps = jnp.clip(jnp.exp(jax.random.uniform(seeds[2], (PAIRS,), jnp.float32, math.log(0.5), math.log(4.0))), 0.5, 4.0)
    omega_values = jnp.clip(jnp.exp(jax.random.uniform(seeds[3], (NFREQ,), jnp.float32, math.log(0.25), math.log(8.0))), 0.25, 8.0)
    quad_weight = jnp.clip(jnp.exp(jax.random.uniform(seeds[4], (NFREQ,), jnp.float32, math.log(0.2), math.log(1.0))), 0.2, 1.0)
    freq_slot = jax.random.permutation(seeds[5], NFREQ).astype(jnp.int32)
    block_list = jax.random.permutation(seeds[6], NBLK).astype(jnp.int32)
    return {"pair_block": pair_block, "screened": screened, "pair_gaps": pair_gaps, "omega_values": omega_values, "quad_weight": quad_weight, "freq_slot": freq_slot, "block_list": block_list}


def reference(pair_block, screened, pair_gaps, omega_values, quad_weight, freq_slot, block_list):
    blocks_all = block_list.shape[0]
    rows_each = pair_gaps.shape[0] // blocks_all
    matches = block_list[:, None] == jnp.arange(blocks_all, dtype=jnp.int32)[None, :]
    gap_table = pair_gaps.reshape(blocks_all, rows_each)
    gap_rows = jnp.sum(jnp.where(matches[:, :, None], gap_table[None, :, :], 0.0), axis=1).reshape(-1)
    slots_all = freq_slot.shape[0]
    slot_match = freq_slot[:, None] == jnp.arange(slots_all, dtype=jnp.int32)[None, :]
    omega_slot = jnp.sum(jnp.where(slot_match, omega_values[None, :], 0.0), axis=1)
    weight_slot = jnp.sum(jnp.where(slot_match, quad_weight[None, :], 0.0), axis=1)
    factor = weight_slot[:, None] * 2.0 * gap_rows[None, :] / (gap_rows[None, :] ** 2 + omega_slot[:, None] ** 2)

    def add_slot(running, inputs):
        matrix, scaled = inputs
        product = jnp.dot(pair_block, matrix, preferred_element_type=jnp.float32)
        return running + scaled[:, None] * product, None

    initial = jnp.zeros((PAIRS, NAUX), jnp.float32)
    result, _ = lax.scan(add_slot, initial, (screened, factor))
    return result
```

```python
import jax
import jax.numpy as jnp
from jax import lax
from jax.experimental import pallas as pl
from jax.experimental.pallas import tpu as pltpu
from jax.sharding import PartitionSpec as P

MESH = pl.DeviceIdType.MESH
F32 = jnp.float32


def kernel(
    b_hbm, w_hbm, gaps_hbm, omega_hbm, weight_hbm, slot_hbm, list_hbm, out_ref,
    b_own, w_ref, gaps, omega, weight, slot, blist, in_sem,
    rows_ref, fac_ref, bg, part, part_in, ys, yr, xs, xr, zs, zr,
    g_send, g_recv, d_send, d_recv, y_send, y_recv, x_send, x_recv, z_send, z_recv,
):
    f, r, c = lax.axis_index("freq"), lax.axis_index("row"), lax.axis_index("col")
    y, zh, core = r // 4, (r // 2) % 2, r % 2
    slots = w_ref.shape[0]

    def at_x(k):
        return ((f + k) % 4, r, c)

    def at_y(k):
        return (f, (r + 4 * k) % 16, c)

    partner = (f, r + 1 - 2 * core, c)
    across = (f, r + 2 - 4 * zh, c)

    barrier = pltpu.get_barrier_semaphore()
    peers = [at_x(1), at_x(3), at_x(2), at_y(1), at_y(3), at_y(2), partner, across]
    for peer in peers:
        pl.semaphore_signal(barrier, inc=1, device_id=peer, device_id_type=MESH)

    small = [
        pltpu.make_async_copy(src, dst, in_sem.at[i])
        for i, (src, dst) in enumerate(
            ((list_hbm, blist), (gaps_hbm, gaps), (slot_hbm, slot), (omega_hbm, omega), (weight_hbm, weight))
        )
    ]
    own = pltpu.make_async_copy(b_hbm, b_own, in_sem.at[5])
    heavy = [pltpu.make_async_copy(w_hbm.at[s], w_ref.at[s], in_sem.at[6 + s]) for s in range(slots)]
    own.start()
    for copy in small + heavy:
        copy.start()

    to = lax.broadcasted_iota(jnp.int32, (192, 192), 0)
    source = lax.broadcasted_iota(jnp.int32, (192, 192), 1)
    half_of = (to >= 96).astype(jnp.int32)
    in_half = to - 96 * half_of
    core_of = (in_half >= 48).astype(jnp.int32)
    in_core = in_half - 48 * core_of
    tail = in_core - 32
    wide_y, wide_i = lax.shift_right_logical(in_core, 3), lax.bitwise_and(in_core, 7)
    tail_y, tail_i = lax.shift_right_logical(jnp.maximum(tail, 0), 2), 8 + lax.bitwise_and(jnp.maximum(tail, 0), 3)
    y_of = jnp.where(tail >= 0, tail_y, wide_y)
    i_of = jnp.where(tail >= 0, tail_i, wide_i)
    z_of = jnp.where(half_of == 0, 1 - zh, zh)
    wanted = y_of * 48 + z_of * 24 + core_of * 12 + i_of
    permute = jnp.where(source == wanted, 1.0, 0.0).astype(jnp.bfloat16)
    own.wait()
    bg[0] = jnp.dot(permute, b_own[...], preferred_element_type=F32).astype(jnp.bfloat16)

    pl.semaphore_wait(barrier, len(peers))

    def gather(k, half):
        rows = pl.ds(96 * half, 96)
        return pltpu.make_async_remote_copy(
            src_ref=bg.at[0, rows], dst_ref=bg.at[k, rows], send_sem=g_send.at[2 * k + half],
            recv_sem=g_recv.at[2 * k + half], device_id=at_x(k), device_id_type=MESH,
        )

    gathers = {(k, half): gather(k, half) for half in range(2) for k in (1, 3, 2)}
    for k in (1, 3, 2):
        gathers[k, 0].start()

    for copy in small:
        copy.wait()

    def fill(n, carry):
        k, half, of_core, of_y = n // 16, (n // 8) % 2, (n // 4) % 2, n % 4
        z = jnp.where(half == 0, 1 - zh, zh)
        block = blist[((f + 4 - k) % 4) * 16 + of_y * 4 + z * 2 + of_core]
        for i in range(12):
            row = of_core * 48 + (of_y * 8 + i if i < 8 else 32 + of_y * 4 + i - 8)
            rows_ref[2 * k + half, pl.ds(row, 1), :] = jnp.full((1, 128), gaps[block * 12 + i], F32)
        return carry

    lax.fori_loop(0, 64, fill, 0)

    def weigh(n, carry):
        gap = rows_ref[n]
        for s in range(slots):
            held = slot[f * slots + s]
            fac_ref[s, n] = weight[held] * 2.0 * gap / (gap * gap + omega[held] * omega[held])
        return carry

    lax.fori_loop(0, 8, weigh, 0)
    for copy in heavy:
        copy.wait()

    def compute(k, half):
        left = bg[k, pl.ds(96 * half, 96), :]

        def tile(n, carry):
            columns = pl.ds(pl.multiple_of(n * 256, 256), 256)
            total = None
            for s in range(slots):
                product = jnp.dot(left, w_ref[s, :, columns], preferred_element_type=F32)
                factor = fac_ref[s, 2 * k + half]
                term = product * jnp.concatenate([factor, factor], axis=1)
                total = term if total is None else total + term
            part[2 * k + half, :, columns] = total
            return carry

        lax.fori_loop(0, w_ref.shape[2] // 256, tile, 0)

    def swap(k, half):
        n = 2 * k + half
        return pltpu.make_async_remote_copy(
            src_ref=part.at[n, pl.ds(pl.multiple_of(48 - 48 * core, 8), 48)], dst_ref=part_in.at[n],
            send_sem=d_send.at[n], recv_sem=d_recv.at[n], device_id=partner, device_id_type=MESH,
        )

    def along_y(k, half, j):
        n = 2 * k + half
        return pltpu.make_async_remote_copy(
            src_ref=ys.at[n, (y + j) % 4], dst_ref=yr.at[n, j - 1], send_sem=y_send.at[n, j - 1],
            recv_sem=y_recv.at[n, j - 1], device_id=at_y(j), device_id_type=MESH,
        )

    def along_x(k, half):
        n = 2 * k + half
        return pltpu.make_async_remote_copy(
            src_ref=xs.at[n], dst_ref=xr.at[n], send_sem=x_send.at[n],
            recv_sem=x_recv.at[n], device_id=at_x(4 - k), device_id_type=MESH,
        )

    low = lax.broadcasted_iota(jnp.int32, (8, 512), 0) < 4

    def to_y(k, half):
        n = 2 * k + half
        swap(k, half).wait_recv()
        both = part[n, pl.ds(pl.multiple_of(48 * core, 8), 48), :] + part_in[n]
        for d in range(4):
            ys[n, d, 0:8] = both[8 * d : 8 * d + 8, :512]
            ys[n, d, 8:16] = both[8 * d : 8 * d + 8, 512:]
            mixed = both[32 + 8 * (d // 2) : 40 + 8 * (d // 2)]
            if d % 2 == 0:
                ys[n, d, 16:24] = jnp.where(low, mixed[:, :512], pltpu.roll(mixed[:, 512:], 4, 0))
            else:
                ys[n, d, 16:24] = jnp.where(low, pltpu.roll(mixed[:, :512], 4, 0), mixed[:, 512:])
        for j in (1, 3, 2):
            along_y(k, half, j).start()

    def to_x(k, half):
        n = 2 * k + half
        for j in (1, 3, 2):
            along_y(k, half, j).wait_recv()
        xs[n] = (ys[n, y] + yr[n, 0]) + (yr[n, 1] + yr[n, 2])
        if k:
            along_x(k, half).start()

    def arrived(half):
        for k in (1, 3, 2):
            along_x(k, half).wait_recv()
        return (xs[half] + xr[2 + half]) + (xr[4 + half] + xr[6 + half])

    def begin(k, half):
        if k:
            gathers[k, half].wait_recv()
        compute(k, half)
        swap(k, half).start()

    begin(0, 0)
    begin(1, 0)
    to_y(0, 0)
    begin(3, 0)
    to_y(1, 0)
    begin(2, 0)
    to_y(3, 0)
    for k in (1, 3, 2):
        gathers[k, 1].start()
    to_y(2, 0)
    to_x(0, 0)
    to_x(1, 0)
    begin(0, 1)
    to_x(3, 0)
    to_x(2, 0)
    zs[...] = arrived(0)
    over = pltpu.make_async_remote_copy(
        src_ref=zs, dst_ref=zr, send_sem=z_send, recv_sem=z_recv, device_id=across, device_id_type=MESH
    )
    over.start()
    to_y(0, 1)
    begin(1, 1)
    begin(3, 1)
    to_y(1, 1)
    begin(2, 1)
    to_y(3, 1)
    to_y(2, 1)
    for k in (0, 1, 3, 2):
        to_x(k, 1)
    kept = arrived(1)
    over.wait_recv()
    total = kept + zr[...]
    out_ref[0:8, :512] = total[0:8]
    out_ref[0:8, 512:] = total[8:16]
    out_ref[8:12, :512] = total[16:20]
    out_ref[8:12, 512:] = pltpu.roll(total[16:24], 4, 0)[0:4]

    for half in range(2):
        for k in range(4):
            swap(k, half).wait_send()
            for j in (1, 2, 3):
                along_y(k, half, j).wait_send()
            if k:
                gathers[k, half].wait_send()
                along_x(k, half).wait_send()
    over.wait_send()


def local(*args):
    dma = pltpu.SemaphoreType.DMA
    hbm = pl.BlockSpec(memory_space=pl.ANY)
    pair_block, screened, pair_gaps, omega_values, quad_weight, freq_slot, block_list = args
    scratch = [
        pltpu.VMEM(pair_block.shape, jnp.bfloat16),
        pltpu.VMEM(screened.shape, jnp.bfloat16),
        pltpu.SMEM(pair_gaps.shape, F32),
        pltpu.SMEM(omega_values.shape, F32),
        pltpu.SMEM(quad_weight.shape, F32),
        pltpu.SMEM(freq_slot.shape, jnp.int32),
        pltpu.SMEM(block_list.shape, jnp.int32),
        dma((10,)),
        pltpu.VMEM((8, 96, 128), F32),
        pltpu.VMEM((4, 8, 96, 128), F32),
        pltpu.VMEM((4, 192, 512), jnp.bfloat16),
        pltpu.VMEM((8, 96, 1024), F32),
        pltpu.VMEM((8, 48, 1024), F32),
        pltpu.VMEM((8, 4, 24, 512), F32),
        pltpu.VMEM((8, 3, 24, 512), F32),
        pltpu.VMEM((8, 24, 512), F32),
        pltpu.VMEM((8, 24, 512), F32),
        pltpu.VMEM((24, 512), F32),
        pltpu.VMEM((24, 512), F32),
        dma((8,)), dma((8,)), dma((8,)), dma((8,)), dma((8, 3)), dma((8, 3)), dma((8,)), dma((8,)),
        dma, dma,
    ]
    return pl.pallas_call(
        kernel,
        out_shape=jax.ShapeDtypeStruct((12, 1024), F32),
        in_specs=[hbm] * 7,
        out_specs=pl.BlockSpec(memory_space=pltpu.VMEM),
        scratch_shapes=scratch,
        compiler_params=pltpu.CompilerParams(collective_id=0, has_side_effects=True),
        name="rpa_exchange",
    )(*args)


def solution(mesh):
    placed = (P("freq", "row"), P("freq", "row", "col"), P(), P(), P(), P(), P())
    return jax.shard_map(
        local, mesh=mesh, in_specs=placed, out_specs=P(("freq", "row"), "col"), check_vma=False
    )
```

```python
import jax
import jax.numpy as jnp
from jax import lax
from jax.experimental import pallas as pl
from jax.experimental.pallas import tpu as pltpu
from jax.sharding import PartitionSpec as P

MESH = pl.DeviceIdType.MESH
F32 = jnp.float32


def kernel(
    b_hbm, w_hbm, gaps_hbm, omega_hbm, weight_hbm, slot_hbm, list_hbm, out_ref,
    b_own, w_ref, gaps, omega, weight, slot, blist, in_sem,
    rows_ref, fac_ref, bg, part, part_in, ys, yq, ysc, yrq, yrs, xs, xq, xsc, xrq, xrs, zq, zsc, zrq, zrs,
    hop, g_send, g_recv, d_send, d_recv, y_send, y_recv, x_send, x_recv, z_send, z_recv,
):
    f, r, c = lax.axis_index("freq"), lax.axis_index("row"), lax.axis_index("col")
    y, zh, core = r // 4, (r // 2) % 2, r % 2
    slots = w_ref.shape[0]

    def at_x(k):
        return ((f + k) % 4, r, c)

    def at_y(k):
        return (f, (r + 4 * k) % 16, c)

    partner = (f, r + 1 - 2 * core, c)
    across = (f, r + 2 - 4 * zh, c)

    def at_z(d):
        z = (zh * 8 + c + d + 16) % 16
        return (f, r + 2 * (z // 8 - zh), z % 8)

    def tell(i, d):
        pl.semaphore_signal(hop.at[i], inc=1, device_id=at_z(d), device_id_type=MESH)

    def encode(x, to, scale):
        top = jnp.maximum(jnp.max(jnp.abs(x), axis=0, keepdims=True), 1e-30)
        to[...] = jnp.round(x * (32767.0 / top)).astype(jnp.int32).astype(jnp.int16)
        scale[...] = top * (1.0 / 32767.0)

    def decode(held, scale):
        return held[...].astype(jnp.int32).astype(F32) * scale[...]

    barrier = pltpu.get_barrier_semaphore()
    peers = [at_x(1), at_x(3), at_x(2), at_y(1), at_y(3), at_y(2), partner, at_z(1), at_z(-1)]
    for peer in peers:
        pl.semaphore_signal(barrier, inc=1, device_id=peer, device_id_type=MESH)

    small = [
        pltpu.make_async_copy(src, dst, in_sem.at[i])
        for i, (src, dst) in enumerate(
            ((list_hbm, blist), (gaps_hbm, gaps), (slot_hbm, slot), (omega_hbm, omega), (weight_hbm, weight))
        )
    ]
    own = pltpu.make_async_copy(b_hbm, b_own, in_sem.at[5])
    heavy = [pltpu.make_async_copy(w_hbm.at[s], w_ref.at[s], in_sem.at[6 + s]) for s in range(slots)]
    own.start()
    for copy in small + heavy:
        copy.start()

    to = lax.broadcasted_iota(jnp.int32, (192, 192), 0)
    source = lax.broadcasted_iota(jnp.int32, (192, 192), 1)
    half_of = (to >= 96).astype(jnp.int32)
    in_half = to - 96 * half_of
    core_of = (in_half >= 48).astype(jnp.int32)
    in_core = in_half - 48 * core_of
    tail = in_core - 32
    wide_y, wide_i = lax.shift_right_logical(in_core, 3), lax.bitwise_and(in_core, 7)
    tail_y, tail_i = lax.shift_right_logical(jnp.maximum(tail, 0), 2), 8 + lax.bitwise_and(jnp.maximum(tail, 0), 3)
    y_of = jnp.where(tail >= 0, tail_y, wide_y)
    i_of = jnp.where(tail >= 0, tail_i, wide_i)
    z_of = jnp.where(half_of == 0, 1 - zh, zh)
    wanted = y_of * 48 + z_of * 24 + core_of * 12 + i_of
    permute = jnp.where(source == wanted, 1.0, 0.0).astype(jnp.bfloat16)
    for copy in small:
        copy.wait()

    def weights(k, half):
        n = 2 * k + half
        z = 1 - zh if half == 0 else zh

        def fill(m, carry):
            of_core, of_y = m // 4, m % 4
            block = blist[((f + 4 - k) % 4) * 16 + of_y * 4 + z * 2 + of_core]
            for i in range(12):
                row = of_core * 48 + (of_y * 8 + i if i < 8 else 32 + of_y * 4 + i - 8)
                rows_ref[n, pl.ds(row, 1), :] = jnp.full((1, 128), gaps[block * 12 + i], F32)
            return carry

        with jax.named_scope(f'fill{k}{half}'):
          lax.fori_loop(0, 8, fill, 0)
          gap = rows_ref[n]
          for s in range(slots):
            held = slot[f * slots + s]
            fac_ref[s, n] = weight[held] * 2.0 * gap / (gap * gap + omega[held] * omega[held])

    own.wait()
    with jax.named_scope('permute'):
      bg[0] = jnp.dot(permute, b_own[...], preferred_element_type=F32).astype(jnp.bfloat16)
    weights(0, 0)

    with jax.named_scope('barrier'):
      pl.semaphore_wait(barrier, len(peers))

    def gather(k, half):
        rows = pl.ds(96 * half, 96)
        return pltpu.make_async_remote_copy(
            src_ref=bg.at[0, rows], dst_ref=bg.at[k, rows], send_sem=g_send.at[2 * k + half],
            recv_sem=g_recv.at[2 * k + half], device_id=at_x(k), device_id_type=MESH,
        )

    gathers = {(k, half): gather(k, half) for half in range(2) for k in (1, 3, 2)}
    for k in (1, 3, 2):
        gathers[k, 0].start()
    tell(0, -1)
    tell(1, 1)
    with jax.named_scope('w_wait'):
      for copy in heavy:
        copy.wait()

    def compute(k, half):
        left = bg[k, pl.ds(96 * half, 96), :]

        def tile(n, carry):
            columns = pl.ds(pl.multiple_of(n * 256, 256), 256)
            total = None
            for s in range(slots):
                product = jnp.dot(left, w_ref[s, :, columns], preferred_element_type=F32)
                factor = fac_ref[s, 2 * k + half]
                term = product * jnp.concatenate([factor, factor], axis=1)
                total = term if total is None else total + term
            part[2 * k + half, :, columns] = total
            return carry

        with jax.named_scope(f'compute{k}{half}'):
          lax.fori_loop(0, w_ref.shape[2] // 256, tile, 0)

    def swap(k, half):
        n = 2 * k + half
        return pltpu.make_async_remote_copy(
            src_ref=part.at[n, pl.ds(pl.multiple_of(48 - 48 * core, 8), 48)], dst_ref=part_in.at[n],
            send_sem=d_send.at[n], recv_sem=d_recv.at[n], device_id=partner, device_id_type=MESH,
        )

    def send(pairs, ssem, rsem, device):
        return [
            pltpu.make_async_remote_copy(
                src_ref=src, dst_ref=dst, send_sem=ssem.at[i], recv_sem=rsem.at[i],
                device_id=device, device_id_type=MESH,
            )
            for i, (src, dst) in enumerate(pairs)
        ]

    def along_y(k, half, j):
        n, d = 2 * k + half, (y + j) % 4
        pairs = ((yq.at[n, d], yrq.at[n, j - 1]), (ysc.at[n, d], yrs.at[n, j - 1]))
        return send(pairs, y_send.at[n, j - 1], y_recv.at[n, j - 1], at_y(j))

    def along_x(k, half):
        n = 2 * k + half
        return send(((xq.at[n], xrq.at[n]), (xsc.at[n], xrs.at[n])), x_send.at[n], x_recv.at[n], at_x(4 - k))

    low = lax.broadcasted_iota(jnp.int32, (8, 512), 0) < 4

    def to_y(k, half):
        n = 2 * k + half
        with jax.named_scope(f'wswap{k}{half}'):
          swap(k, half).wait_recv()
        with jax.named_scope(f'enc{k}{half}'):
          both = part[n, pl.ds(pl.multiple_of(48 * core, 8), 48), :] + part_in[n]
          for d in range(4):
            mixed = both[32 + 8 * (d // 2) : 40 + 8 * (d // 2)]
            if d % 2 == 0:
                mixed = jnp.where(low, mixed[:, :512], pltpu.roll(mixed[:, 512:], 4, 0))
            else:
                mixed = jnp.where(low, pltpu.roll(mixed[:, :512], 4, 0), mixed[:, 512:])
            tiles = [both[8 * d : 8 * d + 8, 256 * i : 256 * i + 256] for i in range(4)]
            piece = jnp.concatenate(tiles + [mixed[:, :256], mixed[:, 256:]], axis=0)
            ys[n, d] = piece
            encode(piece, yq.at[n, d], ysc.at[n, d])
        for j in (1, 3, 2):
            for copy in along_y(k, half, j):
                copy.start()

    def to_x(k, half):
        n = 2 * k + half
        with jax.named_scope(f'wy{k}{half}'):
          for j in (1, 3, 2):
            for copy in along_y(k, half, j):
                copy.wait_recv()
        total = ys[n, y]
        for j in range(3):
            total = total + decode(yrq.at[n, j], yrs.at[n, j])
        if k:
            encode(total, xq.at[n], xsc.at[n])
            for copy in along_x(k, half):
                copy.start()
        else:
            xs[half] = total

    def arrived(half):
        with jax.named_scope(f'wx{half}'):
          for k in (1, 3, 2):
            for copy in along_x(k, half):
                copy.wait_recv()
        total = xs[half]
        for k in (1, 2, 3):
            total = total + decode(xrq.at[2 * k + half], xrs.at[2 * k + half])
        return total

    def begin(k, half):
        if k:
            with jax.named_scope(f'wgather{k}{half}'):
              gathers[k, half].wait_recv()
        compute(k, half)
        swap(k, half).start()

    begin(0, 0)
    for k in (1, 3, 2):
        weights(k, 0)
    to_y(0, 0)
    begin(1, 0)
    pl.semaphore_wait(hop.at[0], 1)
    pl.semaphore_wait(hop.at[1], 1)
    tell(2, -2)
    tell(3, 2)
    begin(3, 0)
    to_y(1, 0)
    begin(2, 0)
    to_y(3, 0)
    for k in (1, 3, 2):
        gathers[k, 1].start()
    for k in (0, 1):
        weights(k, 1)
    to_y(2, 0)
    pl.semaphore_wait(hop.at[2], 1)
    pl.semaphore_wait(hop.at[3], 1)
    tell(4, 4)
    to_x(0, 0)
    begin(0, 1)
    to_x(1, 0)
    begin(1, 1)
    to_x(3, 0)
    to_x(2, 0)
    for k in (3, 2):
        weights(k, 1)
    begin(3, 1)
    total = arrived(0)
    with jax.named_scope('hop'):
      pl.semaphore_wait(hop.at[4], 1)
    encode(total, zq, zsc)
    over = send(((zq, zrq), (zsc, zrs)), z_send, z_recv, across)
    for copy in over:
        copy.start()
    begin(2, 1)
    for k in (0, 1, 3, 2):
        to_y(k, 1)
    for k in (0, 1, 3, 2):
        to_x(k, 1)
    kept = arrived(1)
    with jax.named_scope('wz'):
      for copy in over:
        copy.wait_recv()
    total = kept + decode(zrq, zrs)
    for i in range(4):
        out_ref[0:8, 256 * i : 256 * i + 256] = total[8 * i : 8 * i + 8]
    for i in range(2):
        mixed = total[32 + 8 * i : 40 + 8 * i]
        out_ref[8:12, 256 * i : 256 * i + 256] = mixed[0:4]
        out_ref[8:12, 512 + 256 * i : 768 + 256 * i] = pltpu.roll(mixed, 4, 0)[0:4]

    with jax.named_scope('drain'):
      for half in range(2):
        for k in range(4):
            swap(k, half).wait_send()
            for j in (1, 2, 3):
                for copy in along_y(k, half, j):
                    copy.wait_send()
            if k:
                gathers[k, half].wait_send()
                for copy in along_x(k, half):
                    copy.wait_send()
      for copy in over:
        copy.wait_send()


def local(*args):
    dma = pltpu.SemaphoreType.DMA
    hbm = pl.BlockSpec(memory_space=pl.ANY)
    pair_block, screened, pair_gaps, omega_values, quad_weight, freq_slot, block_list = args
    scratch = [
        pltpu.VMEM(pair_block.shape, jnp.bfloat16),
        pltpu.VMEM(screened.shape, jnp.bfloat16),
        pltpu.SMEM(pair_gaps.shape, F32),
        pltpu.SMEM(omega_values.shape, F32),
        pltpu.SMEM(quad_weight.shape, F32),
        pltpu.SMEM(freq_slot.shape, jnp.int32),
        pltpu.SMEM(block_list.shape, jnp.int32),
        dma((10,)),
        pltpu.VMEM((8, 96, 128), F32),
        pltpu.VMEM((4, 8, 96, 128), F32),
        pltpu.VMEM((4, 192, 512), jnp.bfloat16),
        pltpu.VMEM((8, 96, 1024), F32),
        pltpu.VMEM((8, 48, 1024), F32),
        pltpu.VMEM((8, 4, 48, 256), F32),
        pltpu.VMEM((8, 4, 48, 256), jnp.int16),
        pltpu.VMEM((8, 4, 1, 256), F32),
        pltpu.VMEM((8, 3, 48, 256), jnp.int16),
        pltpu.VMEM((8, 3, 1, 256), F32),
        pltpu.VMEM((2, 48, 256), F32),
        pltpu.VMEM((8, 48, 256), jnp.int16),
        pltpu.VMEM((8, 1, 256), F32),
        pltpu.VMEM((8, 48, 256), jnp.int16),
        pltpu.VMEM((8, 1, 256), F32),
        pltpu.VMEM((48, 256), jnp.int16),
        pltpu.VMEM((1, 256), F32),
        pltpu.VMEM((48, 256), jnp.int16),
        pltpu.VMEM((1, 256), F32),
        pltpu.SemaphoreType.REGULAR((5,)),
        dma((8,)), dma((8,)), dma((8,)), dma((8,)), dma((8, 3, 2)), dma((8, 3, 2)), dma((8, 2)), dma((8, 2)),
        dma((2,)), dma((2,)),
    ]
    return pl.pallas_call(
        kernel,
        out_shape=jax.ShapeDtypeStruct((12, 1024), F32),
        in_specs=[hbm] * 7,
        out_specs=pl.BlockSpec(memory_space=pltpu.VMEM),
        scratch_shapes=scratch,
        compiler_params=pltpu.CompilerParams(collective_id=0, has_side_effects=True),
        name="rpa_exchange",
    )(*args)


def solution(mesh):
    placed = (P("freq", "row"), P("freq", "row", "col"), P(), P(), P(), P(), P())
    return jax.shard_map(
        local, mesh=mesh, in_specs=placed, out_specs=P(("freq", "row"), "col"), check_vma=False
    )
```

```python
import jax
import jax.numpy as jnp
from jax import lax
from jax.experimental import pallas as pl
from jax.experimental.pallas import tpu as pltpu
from jax.sharding import PartitionSpec as P

MESH = pl.DeviceIdType.MESH
F32 = jnp.float32


def kernel(
    b_hbm, w_hbm, gaps_hbm, omega_hbm, weight_hbm, slot_hbm, list_hbm, out_ref,
    b_own, w_ref, gaps, omega, weight, slot, blist, in_sem,
    rows_ref, fac_ref, bg, part, part_in, ys, yq, ysc, yrq, yrs, xs, xq, xsc, xrq, xrs, zq, zsc, zrq, zrs,
    hop, g_send, g_recv, d_send, d_recv, y_send, y_recv, x_send, x_recv, z_send, z_recv,
):
    f, r, c = lax.axis_index("freq"), lax.axis_index("row"), lax.axis_index("col")
    y, zh, core = r // 4, (r // 2) % 2, r % 2
    slots = w_ref.shape[0]

    def at_x(k):
        return ((f + k) % 4, r, c)

    def at_y(k):
        return (f, (r + 4 * k) % 16, c)

    partner = (f, r + 1 - 2 * core, c)
    across = (f, r + 2 - 4 * zh, c)

    def at_z(d):
        z = (zh * 8 + c + d + 16) % 16
        return (f, r + 2 * (z // 8 - zh), z % 8)

    def tell(i, d):
        pl.semaphore_signal(hop.at[i], inc=1, device_id=at_z(d), device_id_type=MESH)

    def encode(x, to, scale):
        top = jnp.maximum(jnp.max(jnp.abs(x), axis=0, keepdims=True), 1e-30)
        to[...] = jnp.round(x * (32767.0 / top)).astype(jnp.int32).astype(jnp.int16)
        scale[...] = top * (1.0 / 32767.0)

    def decode(held, scale):
        return held[...].astype(jnp.int32).astype(F32) * scale[...]

    barrier = pltpu.get_barrier_semaphore()
    peers = [at_x(1), at_x(3), at_x(2), at_y(1), at_y(3), at_y(2), partner, at_z(1), at_z(-1)]
    for peer in peers:
        pl.semaphore_signal(barrier, inc=1, device_id=peer, device_id_type=MESH)

    small = [
        pltpu.make_async_copy(src, dst, in_sem.at[i])
        for i, (src, dst) in enumerate(
            ((list_hbm, blist), (gaps_hbm, gaps), (slot_hbm, slot), (omega_hbm, omega), (weight_hbm, weight))
        )
    ]
    own = pltpu.make_async_copy(b_hbm, b_own, in_sem.at[5])
    heavy = [pltpu.make_async_copy(w_hbm.at[s], w_ref.at[s], in_sem.at[6 + s]) for s in range(slots)]
    own.start()
    for copy in small + heavy:
        copy.start()

    to = lax.broadcasted_iota(jnp.int32, (192, 192), 0)
    source = lax.broadcasted_iota(jnp.int32, (192, 192), 1)
    half_of = (to >= 96).astype(jnp.int32)
    in_half = to - 96 * half_of
    core_of = (in_half >= 48).astype(jnp.int32)
    in_core = in_half - 48 * core_of
    tail = in_core - 32
    wide_y, wide_i = lax.shift_right_logical(in_core, 3), lax.bitwise_and(in_core, 7)
    tail_y, tail_i = lax.shift_right_logical(jnp.maximum(tail, 0), 2), 8 + lax.bitwise_and(jnp.maximum(tail, 0), 3)
    y_of = jnp.where(tail >= 0, tail_y, wide_y)
    i_of = jnp.where(tail >= 0, tail_i, wide_i)
    z_of = jnp.where(half_of == 0, 1 - zh, zh)
    wanted = y_of * 48 + z_of * 24 + core_of * 12 + i_of
    permute = jnp.where(source == wanted, 1.0, 0.0).astype(jnp.bfloat16)
    for copy in small:
        copy.wait()

    def weights(k, half):
        n = 2 * k + half
        z = 1 - zh if half == 0 else zh

        def fill(m, carry):
            of_core, of_y = m // 4, m % 4
            block = blist[((f + 4 - k) % 4) * 16 + of_y * 4 + z * 2 + of_core]
            for i in range(12):
                row = of_core * 48 + (of_y * 8 + i if i < 8 else 32 + of_y * 4 + i - 8)
                rows_ref[n, pl.ds(row, 1), :] = jnp.full((1, 128), gaps[block * 12 + i], F32)
            return carry

        with jax.named_scope(f'fill{k}{half}'):
          lax.fori_loop(0, 8, fill, 0)
          gap = rows_ref[n]
          for s in range(slots):
            held = slot[f * slots + s]
            fac_ref[s, n] = weight[held] * 2.0 * gap / (gap * gap + omega[held] * omega[held])

    own.wait()
    with jax.named_scope('permute'):
      bg[0] = jnp.dot(permute, b_own[...], preferred_element_type=F32).astype(jnp.bfloat16)
    weights(0, 0)

    with jax.named_scope('barrier'):
      pl.semaphore_wait(barrier, len(peers))

    def gather(k, half):
        rows = pl.ds(96 * half, 96)
        return pltpu.make_async_remote_copy(
            src_ref=bg.at[0, rows], dst_ref=bg.at[k, rows], send_sem=g_send.at[2 * k + half],
            recv_sem=g_recv.at[2 * k + half], device_id=at_x(k), device_id_type=MESH,
        )

    gathers = {(k, half): gather(k, half) for half in range(2) for k in (1, 3, 2)}
    for k in (1, 3, 2):
        gathers[k, 0].start()
    tell(0, -1)
    tell(1, 1)
    with jax.named_scope('w_wait'):
      for copy in heavy:
        copy.wait()

    def compute(*blocks):
        left = jnp.concatenate([bg[k, 96 * half : 96 * half + 96] for k, half in blocks], axis=0)

        def tile(n, carry):
            columns = pl.ds(pl.multiple_of(n * 256, 256), 256)
            totals = [None] * len(blocks)
            for s in range(slots):
                product = jnp.dot(left, w_ref[s, :, columns], preferred_element_type=F32)
                for i, (k, half) in enumerate(blocks):
                    factor = fac_ref[s, 2 * k + half]
                    term = product[96 * i : 96 * i + 96] * jnp.concatenate([factor, factor], axis=1)
                    totals[i] = term if totals[i] is None else totals[i] + term
            for (k, half), total in zip(blocks, totals):
                part[2 * k + half, :, columns] = total
            return carry

        with jax.named_scope('compute' + ''.join(f'{k}{half}' for k, half in blocks)):
            lax.fori_loop(0, w_ref.shape[2] // 256, tile, 0)
        for block in blocks:
            swap(*block).start()

    def swap(k, half):
        n = 2 * k + half
        return pltpu.make_async_remote_copy(
            src_ref=part.at[n, pl.ds(pl.multiple_of(48 - 48 * core, 8), 48)], dst_ref=part_in.at[n],
            send_sem=d_send.at[n], recv_sem=d_recv.at[n], device_id=partner, device_id_type=MESH,
        )

    def send(pairs, ssem, rsem, device):
        return [
            pltpu.make_async_remote_copy(
                src_ref=src, dst_ref=dst, send_sem=ssem.at[i], recv_sem=rsem.at[i],
                device_id=device, device_id_type=MESH,
            )
            for i, (src, dst) in enumerate(pairs)
        ]

    def along_y(k, half, j):
        n, d = 2 * k + half, (y + j) % 4
        pairs = ((yq.at[n, d], yrq.at[n, j - 1]), (ysc.at[n, d], yrs.at[n, j - 1]))
        return send(pairs, y_send.at[n, j - 1], y_recv.at[n, j - 1], at_y(j))

    def along_x(k, half):
        n = 2 * k + half
        return send(((xq.at[n], xrq.at[n]), (xsc.at[n], xrs.at[n])), x_send.at[n], x_recv.at[n], at_x(4 - k))

    low = lax.broadcasted_iota(jnp.int32, (8, 512), 0) < 4

    def to_y(k, half):
        n = 2 * k + half
        with jax.named_scope(f'wswap{k}{half}'):
          swap(k, half).wait_recv()
        with jax.named_scope(f'enc{k}{half}'):
          both = part[n, pl.ds(pl.multiple_of(48 * core, 8), 48), :] + part_in[n]
          for d in range(4):
            mixed = both[32 + 8 * (d // 2) : 40 + 8 * (d // 2)]
            if d % 2 == 0:
                mixed = jnp.where(low, mixed[:, :512], pltpu.roll(mixed[:, 512:], 4, 0))
            else:
                mixed = jnp.where(low, pltpu.roll(mixed[:, :512], 4, 0), mixed[:, 512:])
            tiles = [both[8 * d : 8 * d + 8, 256 * i : 256 * i + 256] for i in range(4)]
            piece = jnp.concatenate(tiles + [mixed[:, :256], mixed[:, 256:]], axis=0)
            ys[n, d] = piece
            encode(piece, yq.at[n, d], ysc.at[n, d])
        for j in (1, 3, 2):
            for copy in along_y(k, half, j):
                copy.start()

    def to_x(k, half):
        n = 2 * k + half
        with jax.named_scope(f'wy{k}{half}'):
          for j in (1, 3, 2):
            for copy in along_y(k, half, j):
                copy.wait_recv()
        total = ys[n, y]
        for j in range(3):
            total = total + decode(yrq.at[n, j], yrs.at[n, j])
        if k:
            encode(total, xq.at[n], xsc.at[n])
            for copy in along_x(k, half):
                copy.start()
        else:
            xs[half] = total

    def arrived(half):
        with jax.named_scope(f'wx{half}'):
          for k in (1, 3, 2):
            for copy in along_x(k, half):
                copy.wait_recv()
        total = xs[half]
        for k in (1, 2, 3):
            total = total + decode(xrq.at[2 * k + half], xrs.at[2 * k + half])
        return total

    def gathered(*blocks):
        for k, half in blocks:
            with jax.named_scope(f'wgather{k}{half}'):
                gathers[k, half].wait_recv()

    weights(0, 1)
    compute((0, 0), (0, 1))
    for k in (1, 3, 2):
        weights(k, 0)
    to_y(0, 0)
    gathered((1, 0), (3, 0))
    for k in (1, 3, 2):
        gathers[k, 1].start()
    compute((1, 0), (3, 0))
    pl.semaphore_wait(hop.at[0], 1)
    pl.semaphore_wait(hop.at[1], 1)
    tell(2, -2)
    tell(3, 2)
    to_y(0, 1)
    gathered((2, 0))
    compute((2, 0))
    to_y(1, 0)
    to_y(3, 0)
    for k in (1, 3, 2):
        weights(k, 1)
    to_y(2, 0)
    pl.semaphore_wait(hop.at[2], 1)
    pl.semaphore_wait(hop.at[3], 1)
    tell(4, 4)
    to_x(0, 0)
    gathered((1, 1), (3, 1), (2, 1))
    compute((1, 1), (3, 1), (2, 1))
    to_x(1, 0)
    to_x(3, 0)
    to_x(2, 0)
    for k in (1, 3, 2):
        to_y(k, 1)
    total = arrived(0)
    with jax.named_scope('hop'):
      pl.semaphore_wait(hop.at[4], 1)
    encode(total, zq, zsc)
    over = send(((zq, zrq), (zsc, zrs)), z_send, z_recv, across)
    for copy in over:
        copy.start()
    for k in (0, 1, 3, 2):
        to_x(k, 1)
    kept = arrived(1)
    with jax.named_scope('wz'):
      for copy in over:
        copy.wait_recv()
    total = kept + decode(zrq, zrs)
    for i in range(4):
        out_ref[0:8, 256 * i : 256 * i + 256] = total[8 * i : 8 * i + 8]
    for i in range(2):
        mixed = total[32 + 8 * i : 40 + 8 * i]
        out_ref[8:12, 256 * i : 256 * i + 256] = mixed[0:4]
        out_ref[8:12, 512 + 256 * i : 768 + 256 * i] = pltpu.roll(mixed, 4, 0)[0:4]

    with jax.named_scope('drain'):
      for half in range(2):
        for k in range(4):
            swap(k, half).wait_send()
            for j in (1, 2, 3):
                for copy in along_y(k, half, j):
                    copy.wait_send()
            if k:
                gathers[k, half].wait_send()
                for copy in along_x(k, half):
                    copy.wait_send()
      for copy in over:
        copy.wait_send()


def local(*args):
    dma = pltpu.SemaphoreType.DMA
    hbm = pl.BlockSpec(memory_space=pltpu.HBM)
    pair_block, screened, pair_gaps, omega_values, quad_weight, freq_slot, block_list = args
    scratch = [
        pltpu.VMEM(pair_block.shape, jnp.bfloat16),
        pltpu.VMEM(screened.shape, jnp.bfloat16),
        pltpu.SMEM(pair_gaps.shape, F32),
        pltpu.SMEM(omega_values.shape, F32),
        pltpu.SMEM(quad_weight.shape, F32),
        pltpu.SMEM(freq_slot.shape, jnp.int32),
        pltpu.SMEM(block_list.shape, jnp.int32),
        dma((10,)),
        pltpu.VMEM((8, 96, 128), F32),
        pltpu.VMEM((4, 8, 96, 128), F32),
        pltpu.VMEM((4, 192, 512), jnp.bfloat16),
        pltpu.VMEM((8, 96, 1024), F32),
        pltpu.VMEM((8, 48, 1024), F32),
        pltpu.VMEM((8, 4, 48, 256), F32),
        pltpu.VMEM((8, 4, 48, 256), jnp.int16),
        pltpu.VMEM((8, 4, 1, 256), F32),
        pltpu.VMEM((8, 3, 48, 256), jnp.int16),
        pltpu.VMEM((8, 3, 1, 256), F32),
        pltpu.VMEM((2, 48, 256), F32),
        pltpu.VMEM((8, 48, 256), jnp.int16),
        pltpu.VMEM((8, 1, 256), F32),
        pltpu.VMEM((8, 48, 256), jnp.int16),
        pltpu.VMEM((8, 1, 256), F32),
        pltpu.VMEM((48, 256), jnp.int16),
        pltpu.VMEM((1, 256), F32),
        pltpu.VMEM((48, 256), jnp.int16),
        pltpu.VMEM((1, 256), F32),
        pltpu.SemaphoreType.REGULAR((5,)),
        dma((8,)), dma((8,)), dma((8,)), dma((8,)), dma((8, 3, 2)), dma((8, 3, 2)), dma((8, 2)), dma((8, 2)),
        dma((2,)), dma((2,)),
    ]
    return pl.pallas_call(
        kernel,
        out_shape=jax.ShapeDtypeStruct((12, 1024), F32),
        in_specs=[hbm] * 7,
        out_specs=pl.BlockSpec(memory_space=pltpu.VMEM),
        scratch_shapes=scratch,
        compiler_params=pltpu.CompilerParams(collective_id=0, has_side_effects=True, vmem_limit_bytes=20 << 20),
        name="rpa_exchange",
    )(*(pltpu.with_memory_space_constraint(a, pltpu.HBM) for a in args))


def solution(mesh):
    placed = (P("freq", "row"), P("freq", "row", "col"), P(), P(), P(), P(), P())
    return jax.shard_map(
        local, mesh=mesh, in_specs=placed, out_specs=P(("freq", "row"), "col"), check_vma=False
    )
```

```python
import jax
import jax.numpy as jnp
from jax import lax
from jax.experimental import pallas as pl
from jax.experimental.pallas import tpu as pltpu
from jax.sharding import PartitionSpec as P

MESH = pl.DeviceIdType.MESH
F32 = jnp.float32


def kernel(
    b_hbm, w_hbm, gaps_hbm, omega_hbm, weight_hbm, slot_hbm, list_hbm, out_ref,
    b_own, w_ref, gaps, omega, weight, slot, blist, in_sem,
    rows_ref, fac_ref, bg, part, part_in, ys, yq, ysc, yrq, yrs, xs, xq, xsc, xrq, xrs, zq, zsc, zrq, zrs,
    hop, g_send, g_recv, d_send, d_recv, y_send, y_recv, x_send, x_recv, z_send, z_recv,
):
    f, r, c = lax.axis_index("freq"), lax.axis_index("row"), lax.axis_index("col")
    y, zh, core = r // 4, (r // 2) % 2, r % 2
    slots = w_ref.shape[0]

    def at_x(k):
        return ((f + k) % 4, r, c)

    def at_y(k):
        return (f, (r + 4 * k) % 16, c)

    partner = (f, r + 1 - 2 * core, c)
    across = (f, r + 2 - 4 * zh, c)

    def at_z(d):
        z = (zh * 8 + c + d + 16) % 16
        return (f, r + 2 * (z // 8 - zh), z % 8)

    def tell(i, d):
        pl.semaphore_signal(hop.at[i], inc=1, device_id=at_z(d), device_id_type=MESH)

    def encode(x, to, scale):
        top = jnp.maximum(jnp.max(jnp.abs(x), axis=0, keepdims=True), 1e-30)
        to[...] = jnp.round(x * (32767.0 / top)).astype(jnp.int32).astype(jnp.int16)
        scale[...] = top * (1.0 / 32767.0)

    def decode(held, scale):
        return held[...].astype(jnp.int32).astype(F32) * scale[...]

    zpos = zh * 8 + c
    barrier = pltpu.get_barrier_semaphore()
    peers = [at_x(1), at_x(3), at_x(2), at_y(1), at_y(3), at_y(2), partner]
    for peer in peers:
        pl.semaphore_signal(barrier, inc=1, device_id=peer, device_id_type=MESH)
    for d, there in ((1, zpos < 15), (-1, zpos > 0)):

        @pl.when(there)
        def _():
            pl.semaphore_signal(barrier, inc=1, device_id=at_z(d), device_id_type=MESH)

    def between(low, high):
        return pl.when(jnp.logical_and(zpos >= low, zpos <= high))

    def learn(step):
        if step == 1:
            between(1, 12)(lambda: tell(0, 1))
            between(3, 14)(lambda: tell(1, -1))
        elif step == 2:

            @between(2, 13)
            def _():
                pl.semaphore_wait(hop.at[0], 1)
                pl.semaphore_wait(hop.at[1], 1)

            between(2, 9)(lambda: tell(2, 2))
            between(6, 13)(lambda: tell(3, -2))
        elif step == 3:

            @between(4, 11)
            def _():
                pl.semaphore_wait(hop.at[2], 1)
                pl.semaphore_wait(hop.at[3], 1)
                tell(4, 4)
                tell(4, -4)

        else:
            pl.semaphore_wait(hop.at[4], 1)

    small = [
        pltpu.make_async_copy(src, dst, in_sem.at[i])
        for i, (src, dst) in enumerate(
            ((list_hbm, blist), (gaps_hbm, gaps), (slot_hbm, slot), (omega_hbm, omega), (weight_hbm, weight))
        )
    ]
    own = pltpu.make_async_copy(b_hbm, b_own, in_sem.at[5])
    heavy = [pltpu.make_async_copy(w_hbm.at[s], w_ref.at[s], in_sem.at[6 + s]) for s in range(slots)]
    own.start()
    for copy in small + heavy:
        copy.start()

    to = lax.broadcasted_iota(jnp.int32, (192, 192), 0)
    source = lax.broadcasted_iota(jnp.int32, (192, 192), 1)
    half_of = (to >= 96).astype(jnp.int32)
    in_half = to - 96 * half_of
    core_of = (in_half >= 48).astype(jnp.int32)
    in_core = in_half - 48 * core_of
    tail = in_core - 32
    wide_y, wide_i = lax.shift_right_logical(in_core, 3), lax.bitwise_and(in_core, 7)
    tail_y, tail_i = lax.shift_right_logical(jnp.maximum(tail, 0), 2), 8 + lax.bitwise_and(jnp.maximum(tail, 0), 3)
    y_of = jnp.where(tail >= 0, tail_y, wide_y)
    i_of = jnp.where(tail >= 0, tail_i, wide_i)
    z_of = jnp.where(half_of == 0, 1 - zh, zh)
    wanted = y_of * 48 + z_of * 24 + core_of * 12 + i_of
    permute = jnp.where(source == wanted, 1.0, 0.0).astype(jnp.bfloat16)
    for copy in small:
        copy.wait()

    def weights(k, half):
        n = 2 * k + half
        z = 1 - zh if half == 0 else zh

        def fill(m, carry):
            of_core, of_y = m // 4, m % 4
            block = blist[((f + 4 - k) % 4) * 16 + of_y * 4 + z * 2 + of_core]
            for i in range(12):
                row = of_core * 48 + (of_y * 8 + i if i < 8 else 32 + of_y * 4 + i - 8)
                rows_ref[n, pl.ds(row, 1), :] = jnp.full((1, 128), gaps[block * 12 + i], F32)
            return carry

        with jax.named_scope(f'fill{k}{half}'):
          lax.fori_loop(0, 8, fill, 0)
          gap = rows_ref[n]
          for s in range(slots):
            held = slot[f * slots + s]
            fac_ref[s, n] = weight[held] * 2.0 * gap / (gap * gap + omega[held] * omega[held])

    own.wait()
    with jax.named_scope('permute'):
      bg[0] = jnp.dot(permute, b_own[...], preferred_element_type=F32).astype(jnp.bfloat16)
    weights(0, 0)

    with jax.named_scope('barrier'):
      pl.semaphore_wait(barrier, len(peers) + (zpos < 15).astype(jnp.int32) + (zpos > 0).astype(jnp.int32))

    def gather(k, half):
        rows = pl.ds(96 * half, 96)
        return pltpu.make_async_remote_copy(
            src_ref=bg.at[0, rows], dst_ref=bg.at[k, rows], send_sem=g_send,
            recv_sem=g_recv.at[2 * k + half], device_id=at_x(k), device_id_type=MESH,
        )

    gathers = {(k, half): gather(k, half) for half in range(2) for k in (1, 3, 2)}
    for k in (1, 3, 2):
        gathers[k, 0].start()
    learn(1)
    with jax.named_scope('w_wait'):
      for copy in heavy:
        copy.wait()

    def compute(blocks, h):
        left = jnp.concatenate([bg[k, 96 * half : 96 * half + 96] for k, half in blocks], axis=0)

        def tile(n, carry):
            columns = pl.ds(pl.multiple_of(n * 256, 256), 256)
            totals = [None] * len(blocks)
            for s in range(slots):
                product = jnp.dot(left, w_ref[s, :, columns], preferred_element_type=F32)
                for i, (k, half) in enumerate(blocks):
                    factor = fac_ref[s, 2 * k + half]
                    term = product[96 * i : 96 * i + 96] * jnp.concatenate([factor, factor], axis=1)
                    totals[i] = term if totals[i] is None else totals[i] + term
            for (k, half), total in zip(blocks, totals):
                part[2 * k + half, :, columns] = total
            return carry

        with jax.named_scope('compute' + ''.join(f'{k}{half}' for k, half in blocks)):
            lax.fori_loop(2 * h, 2 * h + 2, tile, 0)
        for k, half in blocks:
            swap(k, half, h).start()

    def swap(k, half, h):
        n = 2 * k + half
        columns = pl.ds(512 * h, 512)
        return pltpu.make_async_remote_copy(
            src_ref=part.at[n, pl.ds(pl.multiple_of(48 - 48 * core, 8), 48), columns],
            dst_ref=part_in.at[n, :, columns], send_sem=d_send, recv_sem=d_recv.at[n, h],
            device_id=partner, device_id_type=MESH,
        )

    def send(pairs, ssem, rsem, device):
        return [
            pltpu.make_async_remote_copy(
                src_ref=src, dst_ref=dst, send_sem=ssem.at[i], recv_sem=rsem.at[i],
                device_id=device, device_id_type=MESH,
            )
            for i, (src, dst) in enumerate(pairs)
        ]

    def landed(ref, sem):
        pltpu.make_async_copy(ref, ref, sem).wait()

    def along_y(k, half, h, j):
        n, d = 2 * k + half, (y + j) % 4
        pairs = ((yq.at[n, h, d], yrq.at[n, h, j - 1]), (ysc.at[n, h, d], yrs.at[n, h, j - 1]))
        return send(pairs, y_send, y_recv.at[n, h], at_y(j))

    def along_x(k, half, h):
        n = 2 * k + half
        pairs = ((xq.at[n, h], xrq.at[half, h, k - 1]), (xsc.at[n, h], xrs.at[half, h, k - 1]))
        return send(pairs, x_send, x_recv.at[half, h], at_x(4 - k))

    def along_z(h):
        pairs = ((zq.at[h], zrq.at[h]), (zsc.at[h], zrs.at[h]))
        return send(pairs, z_send, z_recv.at[h], across)

    low = lax.broadcasted_iota(jnp.int32, (8, 256), 0) < 4

    def to_y(k, half, h):
        n = 2 * k + half
        with jax.named_scope(f'wswap{k}{half}{h}'):
            swap(k, half, h).wait_recv()
        columns = pl.ds(512 * h, 512)
        both = part[n, pl.ds(pl.multiple_of(48 * core, 8), 48), columns] + part_in[n, :, columns]
        for d in range(4):
            mixed = both[32 + 8 * (d // 2) : 40 + 8 * (d // 2)]
            if d % 2 == 0:
                mixed = jnp.where(low, mixed[:, :256], pltpu.roll(mixed[:, 256:], 4, 0))
            else:
                mixed = jnp.where(low, pltpu.roll(mixed[:, :256], 4, 0), mixed[:, 256:])
            tiles = [both[8 * d : 8 * d + 8, 128 * i : 128 * i + 128] for i in range(4)]
            piece = jnp.concatenate(tiles + [mixed[:, :128], mixed[:, 128:]], axis=0)
            ys[n, h, d] = piece
            encode(piece, yq.at[n, h, d], ysc.at[n, h, d])
        for j in (1, 3, 2):
            for copy in along_y(k, half, h, j):
                copy.start()

    def to_x(k, half, h):
        n = 2 * k + half
        with jax.named_scope(f'wy{k}{half}{h}'):
            landed(yrq.at[n, h], y_recv.at[n, h, 0])
            landed(yrs.at[n, h], y_recv.at[n, h, 1])
        total = ys[n, h, y]
        for j in range(3):
            total = total + decode(yrq.at[n, h, j], yrs.at[n, h, j])
        if k:
            encode(total, xq.at[n, h], xsc.at[n, h])
            for copy in along_x(k, half, h):
                copy.start()
        else:
            xs[half, h] = total

    def arrived(half, h):
        with jax.named_scope(f'wx{half}{h}'):
            landed(xrq.at[half, h], x_recv.at[half, h, 0])
            landed(xrs.at[half, h], x_recv.at[half, h, 1])
        total = xs[half, h]
        for k in range(3):
            total = total + decode(xrq.at[half, h, k], xrs.at[half, h, k])
        return total

    def gathered(*blocks):
        for k, half in blocks:
            with jax.named_scope(f'wgather{k}{half}'):
                gathers[k, half].wait_recv()

    weights(0, 1)
    for h in range(2):
        compute(((0, 0), (0, 1)), h)
    for k in (1, 3, 2):
        weights(k, 0)
    for h in range(2):
        to_y(0, 0, h)
    gathered((1, 0), (3, 0))
    for k in (1, 3, 2):
        gathers[k, 1].start()
    for h in range(2):
        compute(((1, 0), (3, 0)), h)
    learn(2)
    for h in range(2):
        to_y(0, 1, h)
    gathered((2, 0))
    for h in range(2):
        compute(((2, 0),), h)
        to_y(1, 0, h)
        to_y(3, 0, h)
    for h in range(2):
        to_y(2, 0, h)
    for k in (1, 3, 2):
        weights(k, 1)
    learn(3)
    for h in range(2):
        to_x(0, 0, h)
    gathered((1, 1), (3, 1), (2, 1))
    home = ((1, 1), (3, 1), (2, 1))
    compute(home, 0)
    for h in range(2):
        for k in (1, 3):
            to_x(k, 0, h)
    for h in range(2):
        to_x(2, 0, h)
    compute(home, 1)
    for k, half in home:
        to_y(k, half, 0)
    with jax.named_scope('hop'):
        learn(4)
    for h in range(2):
        encode(arrived(0, h), zq.at[h], zsc.at[h])
        for copy in along_z(h):
            copy.start()
    for k, half in home:
        to_y(k, half, 1)
    for h in range(2):
        for k in (0, 1, 3, 2):
            to_x(k, 1, h)
    for h in range(2):
        kept = arrived(1, h)
        with jax.named_scope(f'wz{h}'):
            for copy in along_z(h):
                copy.wait_recv()
        total = kept + decode(zrq.at[h], zrs.at[h])
        for i in range(4):
            out_ref[0:8, 512 * h + 128 * i : 512 * h + 128 * i + 128] = total[8 * i : 8 * i + 8]
        for i in range(2):
            mixed = total[32 + 8 * i : 40 + 8 * i]
            at = 512 * h + 128 * i
            out_ref[8:12, at : at + 128] = mixed[0:4]
            out_ref[8:12, at + 256 : at + 384] = pltpu.roll(mixed, 4, 0)[0:4]

    with jax.named_scope('drain'):
        landed(bg.at[pl.ds(1, 3)], g_send)
        landed(part_in, d_send)
        landed(yrq, y_send.at[0])
        landed(yrs, y_send.at[1])
        landed(xrq, x_send.at[0])
        landed(xrs, x_send.at[1])
        landed(zrq, z_send.at[0])
        landed(zrs, z_send.at[1])


def local(*args):
    dma = pltpu.SemaphoreType.DMA
    hbm = pl.BlockSpec(memory_space=pltpu.HBM)
    pair_block, screened, pair_gaps, omega_values, quad_weight, freq_slot, block_list = args
    scratch = [
        pltpu.VMEM(pair_block.shape, jnp.bfloat16),
        pltpu.VMEM(screened.shape, jnp.bfloat16),
        pltpu.SMEM(pair_gaps.shape, F32),
        pltpu.SMEM(omega_values.shape, F32),
        pltpu.SMEM(quad_weight.shape, F32),
        pltpu.SMEM(freq_slot.shape, jnp.int32),
        pltpu.SMEM(block_list.shape, jnp.int32),
        dma((10,)),
        pltpu.VMEM((8, 96, 128), F32),
        pltpu.VMEM((4, 8, 96, 128), F32),
        pltpu.VMEM((4, 192, 512), jnp.bfloat16),
        pltpu.VMEM((8, 96, 1024), F32),
        pltpu.VMEM((8, 48, 1024), F32),
        pltpu.VMEM((8, 2, 4, 48, 128), F32),
        pltpu.VMEM((8, 2, 4, 48, 128), jnp.int16),
        pltpu.VMEM((8, 2, 4, 1, 128), F32),
        pltpu.VMEM((8, 2, 3, 48, 128), jnp.int16),
        pltpu.VMEM((8, 2, 3, 1, 128), F32),
        pltpu.VMEM((2, 2, 48, 128), F32),
        pltpu.VMEM((8, 2, 48, 128), jnp.int16),
        pltpu.VMEM((8, 2, 1, 128), F32),
        pltpu.VMEM((2, 2, 3, 48, 128), jnp.int16),
        pltpu.VMEM((2, 2, 3, 1, 128), F32),
        pltpu.VMEM((2, 48, 128), jnp.int16),
        pltpu.VMEM((2, 1, 128), F32),
        pltpu.VMEM((2, 48, 128), jnp.int16),
        pltpu.VMEM((2, 1, 128), F32),
        pltpu.SemaphoreType.REGULAR((5,)),
        dma, dma((8,)), dma, dma((8, 2)), dma((2,)), dma((8, 2, 2)),
        dma((2,)), dma((2, 2, 2)), dma((2,)), dma((2, 2)),
    ]
    return pl.pallas_call(
        kernel,
        out_shape=jax.ShapeDtypeStruct((12, 1024), F32),
        in_specs=[hbm] * 7,
        out_specs=pl.BlockSpec(memory_space=pltpu.VMEM),
        scratch_shapes=scratch,
        compiler_params=pltpu.CompilerParams(collective_id=0, has_side_effects=True, vmem_limit_bytes=20 << 20),
        name="rpa_exchange",
    )(*(pltpu.with_memory_space_constraint(a, pltpu.HBM) for a in args))


def solution(mesh):
    placed = (P("freq", "row"), P("freq", "row", "col"), P(), P(), P(), P(), P())
    return jax.shard_map(
        local, mesh=mesh, in_specs=placed, out_specs=P(("freq", "row"), "col"), check_vma=False
    )
```

```python
import jax
import jax.numpy as jnp
from jax import lax
from jax.experimental import pallas as pl
from jax.experimental.pallas import tpu as pltpu
from jax.sharding import PartitionSpec as P

MESH = pl.DeviceIdType.MESH
F32 = jnp.float32


def kernel(
    b_hbm, w_hbm, gaps_hbm, omega_hbm, weight_hbm, slot_hbm, list_hbm, out_ref,
    b_own, w_ref, gaps, omega, weight, slot, blist, in_sem,
    rows_ref, fac_ref, bg, part, part_in, ys, yq, ysc, yrq, yrs, xs, xq, xsc, xrq, xrs, zq, zsc, zrq, zrs,
    hop, g_send, g_recv, d_send, d_recv, y_send, y_recv, x_send, x_recv, z_send, z_recv,
):
    f, r, c = lax.axis_index("freq"), lax.axis_index("row"), lax.axis_index("col")
    y, zh, core = r // 4, (r // 2) % 2, r % 2
    slots = w_ref.shape[0]

    def at_x(k):
        return ((f + k) % 4, r, c)

    def at_y(k):
        return (f, (r + 4 * k) % 16, c)

    partner = (f, r + 1 - 2 * core, c)
    across = (f, r + 2 - 4 * zh, c)

    def at_z(d):
        z = (zh * 8 + c + d + 16) % 16
        return (f, r + 2 * (z // 8 - zh), z % 8)

    def tell(i, d):
        pl.semaphore_signal(hop.at[i], inc=1, device_id=at_z(d), device_id_type=MESH)

    def encode(x, to, scale):
        top = jnp.maximum(jnp.max(jnp.abs(x), axis=0, keepdims=True), 1e-30)
        to[...] = jnp.round(x * (32767.0 / top)).astype(jnp.int32).astype(jnp.int16)
        scale[...] = top * (1.0 / 32767.0)

    def decode(held, scale):
        return held[...].astype(jnp.int32).astype(F32) * scale[...]

    zpos = zh * 8 + c
    barrier = pltpu.get_barrier_semaphore()
    peers = [at_x(1), at_x(3), at_x(2), at_y(1), at_y(3), at_y(2), partner]
    for peer in peers:
        pl.semaphore_signal(barrier, inc=1, device_id=peer, device_id_type=MESH)
    for d, there in ((1, zpos < 15), (-1, zpos > 0)):

        @pl.when(there)
        def _():
            pl.semaphore_signal(barrier, inc=1, device_id=at_z(d), device_id_type=MESH)

    def between(low, high):
        return pl.when(jnp.logical_and(zpos >= low, zpos <= high))

    def learn(step):
        if step == 1:
            between(1, 12)(lambda: tell(0, 1))
            between(3, 14)(lambda: tell(1, -1))
        elif step == 2:

            @between(2, 13)
            def _():
                pl.semaphore_wait(hop.at[0], 1)
                pl.semaphore_wait(hop.at[1], 1)

            between(2, 9)(lambda: tell(2, 2))
            between(6, 13)(lambda: tell(3, -2))
        elif step == 3:

            @between(4, 11)
            def _():
                pl.semaphore_wait(hop.at[2], 1)
                pl.semaphore_wait(hop.at[3], 1)
                tell(4, 4)
                tell(4, -4)

        else:
            pl.semaphore_wait(hop.at[4], 1)

    small = [
        pltpu.make_async_copy(src, dst, in_sem.at[i])
        for i, (src, dst) in enumerate(
            ((list_hbm, blist), (gaps_hbm, gaps), (slot_hbm, slot), (omega_hbm, omega), (weight_hbm, weight))
        )
    ]
    own = pltpu.make_async_copy(b_hbm, b_own, in_sem.at[5])
    heavy = [pltpu.make_async_copy(w_hbm.at[s], w_ref.at[s], in_sem.at[6 + s]) for s in range(slots)]
    own.start()
    for copy in small + heavy:
        copy.start()

    to = lax.broadcasted_iota(jnp.int32, (192, 192), 0)
    source = lax.broadcasted_iota(jnp.int32, (192, 192), 1)
    half_of = (to >= 96).astype(jnp.int32)
    in_half = to - 96 * half_of
    core_of = (in_half >= 48).astype(jnp.int32)
    in_core = in_half - 48 * core_of
    tail = in_core - 32
    wide_y, wide_i = lax.shift_right_logical(in_core, 3), lax.bitwise_and(in_core, 7)
    tail_y, tail_i = lax.shift_right_logical(jnp.maximum(tail, 0), 2), 8 + lax.bitwise_and(jnp.maximum(tail, 0), 3)
    y_of = jnp.where(tail >= 0, tail_y, wide_y)
    i_of = jnp.where(tail >= 0, tail_i, wide_i)
    z_of = jnp.where(half_of == 0, 1 - zh, zh)
    wanted = y_of * 48 + z_of * 24 + core_of * 12 + i_of
    permute = jnp.where(source == wanted, 1.0, 0.0).astype(jnp.bfloat16)
    for copy in small:
        copy.wait()

    def weights(k, half):
        n = 2 * k + half
        z = 1 - zh if half == 0 else zh

        def fill(m, carry):
            of_core, of_y = m // 4, m % 4
            block = blist[((f + 4 - k) % 4) * 16 + of_y * 4 + z * 2 + of_core]
            for i in range(12):
                row = of_core * 48 + (of_y * 8 + i if i < 8 else 32 + of_y * 4 + i - 8)
                rows_ref[n, pl.ds(row, 1), :] = jnp.full((1, 128), gaps[block * 12 + i], F32)
            return carry

        with jax.named_scope(f'fill{k}{half}'):
          lax.fori_loop(0, 8, fill, 0)
          gap = rows_ref[n]
          for s in range(slots):
            held = slot[f * slots + s]
            fac_ref[s, n] = weight[held] * 2.0 * gap / (gap * gap + omega[held] * omega[held])

    own.wait()
    with jax.named_scope('permute'):
      bg[0] = jnp.dot(permute, b_own[...], preferred_element_type=F32).astype(jnp.bfloat16)
    weights(0, 0)

    with jax.named_scope('barrier'):
      pl.semaphore_wait(barrier, len(peers) + (zpos < 15).astype(jnp.int32) + (zpos > 0).astype(jnp.int32))

    def gather(k, half):
        rows = pl.ds(96 * half, 96)
        return pltpu.make_async_remote_copy(
            src_ref=bg.at[0, rows], dst_ref=bg.at[k, rows], send_sem=g_send,
            recv_sem=g_recv.at[2 * k + half], device_id=at_x(k), device_id_type=MESH,
        )

    gathers = {(k, half): gather(k, half) for half in range(2) for k in (1, 3, 2)}
    for k in (1, 3, 2):
        gathers[k, 0].start()
    learn(1)
    with jax.named_scope('w_wait'):
      for copy in heavy:
        copy.wait()

    def compute(blocks, h):
        left = jnp.concatenate([bg[k, 96 * half : 96 * half + 96] for k, half in blocks], axis=0)

        def tile(n, carry):
            columns = pl.ds(pl.multiple_of(n * 256, 256), 256)
            totals = [None] * len(blocks)
            for s in range(slots):
                product = jnp.dot(left, w_ref[s, :, columns], preferred_element_type=F32)
                for i, (k, half) in enumerate(blocks):
                    factor = fac_ref[s, 2 * k + half]
                    term = product[96 * i : 96 * i + 96] * jnp.concatenate([factor, factor], axis=1)
                    totals[i] = term if totals[i] is None else totals[i] + term
            for (k, half), total in zip(blocks, totals):
                part[2 * k + half, :, columns] = total
            return carry

        with jax.named_scope('compute' + ''.join(f'{k}{half}' for k, half in blocks)):
            lax.fori_loop(2 * h, 2 * h + 2, tile, 0)
        for k, half in blocks:
            swap(k, half, h).start()

    def swap(k, half, h):
        n = 2 * k + half
        columns = pl.ds(512 * h, 512)
        return pltpu.make_async_remote_copy(
            src_ref=part.at[n, pl.ds(pl.multiple_of(48 - 48 * core, 8), 48), columns],
            dst_ref=part_in.at[n, :, columns], send_sem=d_send, recv_sem=d_recv.at[n, h],
            device_id=partner, device_id_type=MESH,
        )

    def send(pairs, ssem, rsem, device):
        return [
            pltpu.make_async_remote_copy(
                src_ref=src, dst_ref=dst, send_sem=ssem.at[i], recv_sem=rsem.at[i],
                device_id=device, device_id_type=MESH,
            )
            for i, (src, dst) in enumerate(pairs)
        ]

    def landed(ref, sem):
        pltpu.make_async_copy(ref, ref, sem).wait()

    def along_y(k, half, h, j):
        n, d = 2 * k + half, (y + j) % 4
        pairs = ((yq.at[n, h, d], yrq.at[n, h, j - 1]), (ysc.at[n, h, d], yrs.at[n, h, j - 1]))
        return send(pairs, y_send, y_recv.at[n, h], at_y(j))

    def along_x(k, half, h):
        n = 2 * k + half
        pairs = ((xq.at[n, h], xrq.at[half, h, k - 1]), (xsc.at[n, h], xrs.at[half, h, k - 1]))
        return send(pairs, x_send, x_recv.at[half, h], at_x(4 - k))

    def along_z(h):
        pairs = ((zq.at[h], zrq.at[h]), (zsc.at[h], zrs.at[h]))
        return send(pairs, z_send, z_recv.at[h], across)

    low = lax.broadcasted_iota(jnp.int32, (8, 256), 0) < 4

    def to_y(k, half, h):
        n = 2 * k + half
        with jax.named_scope(f'wswap{k}{half}{h}'):
            swap(k, half, h).wait_recv()
        columns = pl.ds(512 * h, 512)
        both = part[n, pl.ds(pl.multiple_of(48 * core, 8), 48), columns] + part_in[n, :, columns]
        for d in range(4):
            mixed = both[32 + 8 * (d // 2) : 40 + 8 * (d // 2)]
            if d % 2 == 0:
                mixed = jnp.where(low, mixed[:, :256], pltpu.roll(mixed[:, 256:], 4, 0))
            else:
                mixed = jnp.where(low, pltpu.roll(mixed[:, :256], 4, 0), mixed[:, 256:])
            tiles = [both[8 * d : 8 * d + 8, 128 * i : 128 * i + 128] for i in range(4)]
            piece = jnp.concatenate(tiles + [mixed[:, :128], mixed[:, 128:]], axis=0)
            ys[n, h, d] = piece
            encode(piece, yq.at[n, h, d], ysc.at[n, h, d])
        for j in (1, 3, 2):
            for copy in along_y(k, half, h, j):
                copy.start()

    def to_x(k, half, h):
        n = 2 * k + half
        with jax.named_scope(f'wy{k}{half}{h}'):
            landed(yrq.at[n, h], y_recv.at[n, h, 0])
            landed(yrs.at[n, h], y_recv.at[n, h, 1])
        total = ys[n, h, y]
        for j in range(3):
            total = total + decode(yrq.at[n, h, j], yrs.at[n, h, j])
        if k:
            encode(total, xq.at[n, h], xsc.at[n, h])
            for copy in along_x(k, half, h):
                copy.start()
        else:
            xs[half, h] = total

    def arrived(half, h):
        with jax.named_scope(f'wx{half}{h}'):
            landed(xrq.at[half, h], x_recv.at[half, h, 0])
            landed(xrs.at[half, h], x_recv.at[half, h, 1])
        total = xs[half, h]
        for k in range(3):
            total = total + decode(xrq.at[half, h, k], xrs.at[half, h, k])
        return total

    def gathered(*blocks):
        for k, half in blocks:
            with jax.named_scope(f'wgather{k}{half}'):
                gathers[k, half].wait_recv()

    weights(0, 1)
    for h in range(2):
        compute(((0, 0), (0, 1)), h)
    for k in (1, 3, 2):
        weights(k, 0)
    for h in range(2):
        to_y(0, 0, h)
    gathered((1, 0), (3, 0))
    for h in range(2):
        compute(((1, 0), (3, 0)), h)
    learn(2)
    to_y(1, 0, 0)
    to_y(3, 0, 0)
    gathered((2, 0))
    for k in (1, 3, 2):
        gathers[k, 1].start()
    compute(((2, 0),), 0)
    to_y(1, 0, 1)
    to_y(3, 0, 1)
    compute(((2, 0),), 1)
    for h in range(2):
        to_y(2, 0, h)
    for k in (1, 3, 2):
        weights(k, 1)
    learn(3)
    for h in range(2):
        to_x(0, 0, h)
    home = ((1, 1), (3, 1), (2, 1))
    for h in range(2):
        for k in (1, 3):
            to_x(k, 0, h)
    for h in range(2):
        to_x(2, 0, h)
    for h in range(2):
        to_y(0, 1, h)
    gathered(*home)
    compute(home, 0)
    with jax.named_scope('hop'):
        learn(4)
    for h in range(2):
        encode(arrived(0, h), zq.at[h], zsc.at[h])
        for copy in along_z(h):
            copy.start()
    compute(home, 1)
    for h in range(2):
        for k, half in home:
            to_y(k, half, h)
    for h in range(2):
        for k in (0, 1, 3, 2):
            to_x(k, 1, h)
    for h in range(2):
        kept = arrived(1, h)
        with jax.named_scope(f'wz{h}'):
            for copy in along_z(h):
                copy.wait_recv()
        total = kept + decode(zrq.at[h], zrs.at[h])
        for i in range(4):
            out_ref[0:8, 512 * h + 128 * i : 512 * h + 128 * i + 128] = total[8 * i : 8 * i + 8]
        for i in range(2):
            mixed = total[32 + 8 * i : 40 + 8 * i]
            at = 512 * h + 128 * i
            out_ref[8:12, at : at + 128] = mixed[0:4]
            out_ref[8:12, at + 256 : at + 384] = pltpu.roll(mixed, 4, 0)[0:4]

    with jax.named_scope('drain'):
        landed(bg.at[pl.ds(1, 3)], g_send)
        landed(part_in, d_send)
        landed(yrq, y_send.at[0])
        landed(yrs, y_send.at[1])
        landed(xrq, x_send.at[0])
        landed(xrs, x_send.at[1])
        landed(zrq, z_send.at[0])
        landed(zrs, z_send.at[1])


def local(*args):
    dma = pltpu.SemaphoreType.DMA
    hbm = pl.BlockSpec(memory_space=pltpu.HBM)
    pair_block, screened, pair_gaps, omega_values, quad_weight, freq_slot, block_list = args
    scratch = [
        pltpu.VMEM(pair_block.shape, jnp.bfloat16),
        pltpu.VMEM(screened.shape, jnp.bfloat16),
        pltpu.SMEM(pair_gaps.shape, F32),
        pltpu.SMEM(omega_values.shape, F32),
        pltpu.SMEM(quad_weight.shape, F32),
        pltpu.SMEM(freq_slot.shape, jnp.int32),
        pltpu.SMEM(block_list.shape, jnp.int32),
        dma((10,)),
        pltpu.VMEM((8, 96, 128), F32),
        pltpu.VMEM((4, 8, 96, 128), F32),
        pltpu.VMEM((4, 192, 512), jnp.bfloat16),
        pltpu.VMEM((8, 96, 1024), F32),
        pltpu.VMEM((8, 48, 1024), F32),
        pltpu.VMEM((8, 2, 4, 48, 128), F32),
        pltpu.VMEM((8, 2, 4, 48, 128), jnp.int16),
        pltpu.VMEM((8, 2, 4, 1, 128), F32),
        pltpu.VMEM((8, 2, 3, 48, 128), jnp.int16),
        pltpu.VMEM((8, 2, 3, 1, 128), F32),
        pltpu.VMEM((2, 2, 48, 128), F32),
        pltpu.VMEM((8, 2, 48, 128), jnp.int16),
        pltpu.VMEM((8, 2, 1, 128), F32),
        pltpu.VMEM((2, 2, 3, 48, 128), jnp.int16),
        pltpu.VMEM((2, 2, 3, 1, 128), F32),
        pltpu.VMEM((2, 48, 128), jnp.int16),
        pltpu.VMEM((2, 1, 128), F32),
        pltpu.VMEM((2, 48, 128), jnp.int16),
        pltpu.VMEM((2, 1, 128), F32),
        pltpu.SemaphoreType.REGULAR((5,)),
        dma, dma((8,)), dma, dma((8, 2)), dma((2,)), dma((8, 2, 2)),
        dma((2,)), dma((2, 2, 2)), dma((2,)), dma((2, 2)),
    ]
    return pl.pallas_call(
        kernel,
        out_shape=jax.ShapeDtypeStruct((12, 1024), F32),
        in_specs=[hbm] * 7,
        out_specs=pl.BlockSpec(memory_space=pltpu.VMEM),
        scratch_shapes=scratch,
        compiler_params=pltpu.CompilerParams(collective_id=0, has_side_effects=True, vmem_limit_bytes=20 << 20),
        name="rpa_exchange",
    )(*(pltpu.with_memory_space_constraint(a, pltpu.HBM) for a in args))


def solution(mesh):
    placed = (P("freq", "row"), P("freq", "row", "col"), P(), P(), P(), P(), P())
    return jax.shard_map(
        local, mesh=mesh, in_specs=placed, out_specs=P(("freq", "row"), "col"), check_vma=False
    )
```
